32 devices in a mesh: gx: 8 (over z, core), gy: 2 (over y), gz: 2 (over x).
Axes of the slice: x: 2, y: 2, z: 4, core: 2. Of those that a mesh axis runs over, the one named last changes fastest.
Arguments:
- load_current: float32 [384, 4096], P('gy', 'gx'), may hold values from 0 to 90
- sink_mask: int32 [384, 4096], P('gy', 'gx'), may hold values 0 or 1
- pad_mask: int32 [384, 4096], P('gy', 'gx'), may hold values from 0 to 1, as said below
- plane_class: int32 [4, 384, 4096], P('gz', 'gy', 'gx'), may hold values from 0 to 7
- via_class: int32 [4, 384, 4096], P('gz', 'gy', 'gx'), may hold values from 0 to 7
- plane_table: float32 [4, 8], P('gz'), may hold values from 0.25 to 4
- via_table: float32 [4, 8], P('gz'), may hold values from 0.25 to 4
Outputs:
- voltage: float32 [4, 384, 4096], P('gz', 'gy', 'gx')
- residual: float32 [4, 384, 4096], P('gz', 'gy', 'gx')
The draws below stay inside these ranges and needn't reach their ends.
Inputs may be any that keep to these rules, and one draw needn't show every extreme that they name: `pad_mask`: exactly one pad in each aligned 8 x 8 tile of nodes.
All inputs are finite; a program needn't handle non-finite values. No bound on the sum of `sink_mask` on one device may be relied on, other than what follows from the above.
Results may differ from the reference program's by a relative error of at most 0.00012.
Values sent between devices are 32-bit elements; how exact they have to be, the bound alone decides.
A program may use at most 64 MiB of HBM per device.

```python
import math
import jax
import jax.numpy as jnp

L_DEV = 2
ITERS = 3
NCLASS = 8
LAYERS = 4
NX = 4096
NY = 384
N_GZ = 2


def draw_pad_mask(key, part):
    pad_key = jax.random.fold_in(key, 11)
    pad_spots = jax.random.randint(pad_key, (NY // 8, NX // 8), 0, 64)
    row_ids = jnp.arange(NY, dtype=jnp.int32)[:, None]
    col_ids = jnp.arange(NX, dtype=jnp.int32)[None, :]
    local_index = row_ids % 8 * 8 + col_ids % 8
    chosen = jnp.repeat(jnp.repeat(pad_spots, 8, axis=0), 8, axis=1)
    return (local_index == chosen).astype(jnp.int32)


def draw_load_current(key, part):
    base_key = jax.random.fold_in(key, 23)
    row_key, col_key, cell_key = jax.random.split(base_key, 3)
    rise_rows = jnp.arange(NY, dtype=jnp.float32) / NY * math.log(3.0)
    rise_cols = jnp.arange(NX, dtype=jnp.float32) / NX * math.log(3.0)
    log_span = math.log(10.0)
    cell_factor = jnp.exp(jax.random.uniform(cell_key, (NY, NX), jnp.float32, math.log(0.2), math.log(2.0)))
    row_scale = jnp.exp(jax.random.uniform(row_key, (NY, 1), jnp.float32) * log_span + rise_rows[:, None])
    col_scale = jnp.exp(jax.random.uniform(col_key, (1, NX), jnp.float32) * log_span + rise_cols[None, :])
    return (0.02 * row_scale * col_scale * cell_factor).astype(jnp.float32)


def touch_ends(values, rng, low, high):
    dims = values.shape
    spot = [jax.random.randint(jax.random.fold_in(rng, axis), (), 0, dims[axis]) for axis in range(len(dims))]
    values = values.at[tuple(spot)].set(low)
    longest = dims.index(max(dims))
    spot[longest] = (spot[longest] + 1) % dims[longest]
    return values.at[tuple(spot)].set(high)


def shard_levels(own_key, dims, cuts, least, largest):
    factor_of = 1.0
    for dim, blocks in cuts:
        heights = jax.random.uniform(jax.random.fold_in(jax.random.fold_in(own_key, 6), dim), (blocks,), jnp.float32, least / len(cuts), largest / len(cuts))
        factor_of = factor_of * jnp.repeat(jnp.exp(heights), dims[dim] // blocks).reshape((-1,) + (1,) * (len(dims) - 1 - dim))
    return factor_of


def setup_inputs(seed: int = 0) -> dict:
    splits = jax.random.split(jax.random.key(seed), 8)
    load_current = draw_load_current(jax.random.fold_in(splits[7], 71), 0)
    sink_mask = touch_ends((jax.random.randint(splits[1], (NY, NX), 0, 2) < 1).astype(jnp.int32), jax.random.fold_in(splits[1], 1), 0, 1)
    pad_mask = draw_pad_mask(jax.random.fold_in(splits[7], 71), 0)
    plane_class = touch_ends(jax.random.randint(splits[3], (LAYERS, NY, NX), 0, NCLASS), jax.random.fold_in(splits[3], 1), 0, NCLASS - 1).astype(jnp.int32)
    via_class = touch_ends(jax.random.randint(splits[4], (LAYERS, NY, NX), 0, NCLASS), jax.random.fold_in(splits[4], 1), 0, NCLASS - 1).astype(jnp.int32)
    plane_table = jnp.clip(jnp.exp(math.log(4.0) - 2.7725887 * jax.random.uniform(splits[5], (LAYERS, NCLASS), jnp.float32) ** shard_levels(splits[5], (LAYERS, NCLASS), ((0, 2),), -0.2, 0.2)), 0.25, 4.0)
    via_table = jnp.clip(jnp.exp(math.log(4.0) - 2.7725887 * jax.random.uniform(splits[6], (LAYERS, NCLASS), jnp.float32) ** shard_levels(splits[6], (LAYERS, NCLASS), ((0, 2),), -0.2, 0.2)), 0.25, 4.0)
    return {"load_current": load_current, "sink_mask": sink_mask, "pad_mask": pad_mask, "plane_class": plane_class, "via_class": via_class, "plane_table": plane_table, "via_table": via_table}


PAD_CONDUCTANCE = 20.0


def lookup(classes, table):
    summed = jnp.zeros(classes.shape, jnp.float32)
    for level in range(table.shape[1]):
        summed = summed + jnp.where(classes == level, table[:, level][:, None, None], jnp.float32(0.0))
    return summed


def harmonic(first, second):
    return 2.0 * first * second / (first + second)


def factor(diagonal, up_edge):
    inverses = []
    factors = []
    for level in range(diagonal.shape[0]):
        pivots = diagonal[level]
        if level > 0:
            pivots = pivots + up_edge[level - 1] * factors[level - 1]
        inverse = 1.0 / pivots
        inverses.append(inverse)
        factors.append(-up_edge[level] * inverse)
    return jnp.stack(inverses), jnp.stack(factors)


def solve_block(inverses, factors, up_edge, source_term):
    forward = []
    for level in range(source_term.shape[0]):
        entries = source_term[level]
        if level > 0:
            entries = entries + up_edge[level - 1] * forward[level - 1]
        forward.append(entries * inverses[level])
    result = [forward[-1]]
    for level in range(source_term.shape[0] - 2, -1, -1):
        result.insert(0, forward[level] - factors[level] * result[0])
    return jnp.stack(result)


def reference(load_current, sink_mask, pad_mask, plane_class, via_class, plane_table, via_table):
    g_plane = lookup(plane_class, plane_table)
    g_via = lookup(via_class, via_table)
    zero_plane = jnp.zeros((1, NY, NX), jnp.float32)
    east_edge = harmonic(g_plane, jnp.roll(g_plane, -1, 2))
    north_edge = harmonic(g_plane, jnp.roll(g_plane, -1, 1))
    up_edge = jnp.concatenate([harmonic(g_via[:-1], g_via[1:]), zero_plane], 0)
    down_edge = jnp.concatenate([zero_plane, up_edge[:-1]], 0)
    west_edge = jnp.roll(east_edge, 1, 2)
    south_edge = jnp.roll(north_edge, 1, 1)
    pad_layer = jnp.concatenate([jnp.zeros((LAYERS - 1, NY, NX), jnp.float32), (PAD_CONDUCTANCE * pad_mask.astype(jnp.float32))[None]], 0)
    diagonal = east_edge + west_edge + north_edge + south_edge + up_edge + down_edge + pad_layer

    def operate(field):
        above_field = jnp.concatenate([field[1:], zero_plane], 0)
        below_field = jnp.concatenate([zero_plane, field[:-1]], 0)
        return (diagonal * field
                - east_edge * jnp.roll(field, -1, 2) - west_edge * jnp.roll(field, 1, 2)
                - north_edge * jnp.roll(field, -1, 1) - south_edge * jnp.roll(field, 1, 1)
                - up_edge * above_field - down_edge * below_field)

    def blocks(array):
        return array.reshape(N_GZ, L_DEV, NY, NX)

    up_blocks = blocks(up_edge)
    inverses, factors = jax.vmap(factor)(blocks(diagonal), up_blocks)

    def precondition(residual):
        return jax.vmap(solve_block)(inverses, factors, up_blocks, blocks(residual)).reshape(LAYERS, NY, NX)

    source = sink_mask.astype(jnp.float32) * load_current
    right_side = jnp.concatenate([source[None], jnp.zeros((LAYERS - 1, NY, NX), jnp.float32)], 0)
    voltage = jnp.zeros((LAYERS, NY, NX), jnp.float32)
    residual = right_side
    precond = precondition(residual)
    direction = precond
    weight_now = jnp.sum(residual * precond)
    for iteration in range(ITERS):
        image_field = operate(direction)
        step_size = weight_now / jnp.sum(direction * image_field)
        voltage = voltage + step_size * direction
        residual = residual - step_size * image_field
        if iteration + 1 < ITERS:
            precond = precondition(residual)
            weight_next = jnp.sum(residual * precond)
            direction = precond + (weight_next / weight_now) * direction
            weight_now = weight_next
    return voltage, residual
```

```python
import functools

import jax
import jax.numpy as jnp
from jax import lax
from jax.experimental import pallas as pl
from jax.experimental.pallas import tpu as pltpu
from jax.sharding import PartitionSpec as P

PAD_CONDUCTANCE = 20.0
MESH = pl.DeviceIdType.MESH
VMEM = pltpu.VMEM
LANES = 128
SUB = 8
OUTER, INNER = 0, 1


def word_plan(sizes):
    n_gx, n_gy, _ = sizes
    plan, reach = [], 1
    while reach < n_gx // 2:
        plan.append(("gx", reach))
        reach *= 2
    stride = 1
    while stride - 1 < n_gy // 2:
        plan.append(("gy", stride))
        stride *= 2
    return plan


def kernel(
    sizes, chunks,
    load_hbm, sink_hbm, pad_hbm, plane_hbm, via_hbm, plane_tab, via_tab,
    volt, res,
    load, sink, pad, plane, via,
    rv, rvx, rp, edge, dsum, ux, u_in, m, b, z0, z1, z2, zx, n0, n1, n2,
    rows_out, rows_in, cols_out, cols_in, side, acc, part, red1,
    load_sem, p_send, p_recv, h_send, h_recv, s1, r1, ready,
):
    z, n = (z0, z1, z2), (n0, n1, n2)
    n_gx, n_gy, n_gz = sizes
    _, n_rows, n_cols = plane.shape
    groups = n_rows // SUB
    per = groups // chunks
    early = chunks // 2
    span = per * SUB
    last = n_cols - LANES
    gx, gy, gz = lax.axis_index("gx"), lax.axis_index("gy"), lax.axis_index("gz")
    is_bottom = gz == 0
    is_top = gz == n_gz - 1
    layer = {OUTER: gz, INNER: 1 - gz}
    partner = {"gz": 1 - gz}
    east, west = {"gx": lax.rem(gx + 1, n_gx)}, {"gx": lax.rem(gx + n_gx - 1, n_gx)}
    north, south = {"gy": lax.rem(gy + 1, n_gy)}, {"gy": lax.rem(gy + n_gy - 1, n_gy)}

    loads = [
        pltpu.make_async_copy(src, dst, load_sem.at[i])
        for i, (src, dst) in enumerate(
            (
                (via_hbm.at[layer[INNER]], via.at[layer[INNER]]), (plane_hbm, plane),
                (via_hbm.at[layer[OUTER]], via.at[layer[OUTER]]),
                (pad_hbm, pad), (load_hbm, load), (sink_hbm, sink),
            )
        )
    ]
    for copy in loads:
        copy.start()

    total_count = n_gx * n_gy * n_gz
    mine = (gx * n_gy + gy) * n_gz + gz
    everyone = []
    for d in range(1, total_count):
        other = lax.rem(mine + d, total_count)
        everyone.append({
            "gx": other // (n_gy * n_gz), "gy": lax.rem(other // n_gz, n_gy),
            "gz": lax.rem(other, n_gz),
        })

    def around(axis, at, size, stride):
        ahead = {axis: lax.rem(at + stride, size)}
        behind = {axis: lax.rem(at + size - stride, size)}
        return [ahead] if 2 * stride == size else [ahead, behind]

    nearby = [partner] + around("gy", gy, n_gy, 1) + around("gx", gx, n_gx, 1)
    barrier = pltpu.get_barrier_semaphore()
    for peer in nearby:
        pl.semaphore_signal(barrier, inc=1, device_id=peer, device_id_type=MESH)

    stages = [around(axis, at, size, stride) for axis, at, size, stride in (
        ("gx", gx, n_gx, s) if a == "gx" else ("gy", gy, n_gy, s) for a, s in word_plan(sizes)
    )] + [[partner]]
    told = [0]

    def spread():
        if 0 < told[0] <= len(stages):
            pl.semaphore_wait(ready.at[told[0] - 1], len(stages[told[0] - 1]))
        if told[0] < len(stages):
            for peer in stages[told[0]]:
                pl.semaphore_signal(
                    ready.at[told[0]], inc=1, device_id=peer, device_id_type=MESH
                )
        told[0] += 1

    lane = lax.broadcasted_iota(jnp.int32, (SUB, LANES), 1)
    wide = lax.broadcasted_iota(jnp.int32, (SUB, n_cols), 0)
    acc[...] = jnp.zeros_like(acc)
    cols_out[...] = jnp.zeros_like(cols_out)
    rows_out[...] = jnp.zeros_like(rows_out)

    def tile(j):
        return pl.ds(pl.multiple_of(j * SUB, SUB), SUB)

    def inside(j):
        return pl.ds(pl.multiple_of(j * SUB + SUB, SUB), SUB)

    def each(first, count, body, unroll=1):
        def step(i, carry):
            for u in range(wide_step):
                body(first + i * wide_step + u)
            return carry

        wide_step = unroll if count % unroll == 0 else 1
        lax.fori_loop(0, count // wide_step, step, 0)

    def halves(table, which):
        row = 0.5 / table[pl.ds(layer[which], 1), :]
        return [jnp.broadcast_to(row[:, k:k + 1], (SUB, LANES)) for k in range(table.shape[1])]

    def pick(classes, values):
        out = []
        for s in range(0, n_cols, LANES):
            c = classes[:, s:s + LANES]
            level = list(values)
            bit = 1
            while len(level) > 1:
                on = (c & bit) != 0
                level = [jnp.where(on, level[i + 1], level[i]) for i in range(0, len(level), 2)]
                bit *= 2
            out.append(level[0])
        return jnp.concatenate(out, axis=1)

    def fold(x):
        total = x[:, :LANES]
        for s in range(LANES, n_cols, LANES):
            total = total + x[:, s:s + LANES]
        return total

    def plane_copy(e, c, src, dst):
        return pltpu.make_async_remote_copy(
            src_ref=src, dst_ref=dst, send_sem=p_send.at[e, c], recv_sem=p_recv.at[e, c],
            device_id=partner, device_id_type=MESH,
        )

    def chunk(c):
        return pl.ds(c * span, span)

    def via_copy(c):
        return plane_copy(0, c, rv.at[chunk(c)], rvx.at[chunk(c)])

    def field_copy(k, c):
        return plane_copy(
            k + 1, c, z[k].at[INNER, pl.ds(SUB + c * span, span)], zx.at[k, chunk(c)]
        )

    def save_cols(e, which, j, tiles):
        rows = pl.ds(which * SUB, SUB)
        here = lane == j
        right = pltpu.roll(tiles[:, last:], j + 1, 1)
        left = pltpu.roll(tiles[:, :LANES], j, 1)
        cols_out[e, 0, rows] = jnp.where(here, right, cols_out[e, 0, rows])
        cols_out[e, 1, rows] = jnp.where(here, left, cols_out[e, 1, rows])

    def halo_copies(e):
        made = []
        plan = (
            (rows_out.at[e, 0], rows_in.at[e, 0], north),
            (rows_out.at[e, 1], rows_in.at[e, 1], south),
            (cols_out.at[e, 0], cols_in.at[e, 0], east),
            (cols_out.at[e, 1], cols_in.at[e, 1], west),
        )
        for i, (src, dst, peer) in enumerate(plan):
            made.append(
                pltpu.make_async_remote_copy(
                    src_ref=src, dst_ref=dst, send_sem=h_send.at[e, i],
                    recv_sem=h_recv.at[e, i], device_id=peer, device_id_type=MESH,
                )
            )
        return made

    def save_rows(e, field):
        for which in (OUTER, INNER):
            rows_out[e, 0, which:which + 1] = field[which, SUB + n_rows - 1:SUB + n_rows]
            rows_out[e, 1, which:which + 1] = field[which, SUB:SUB + 1]

    def send_halo(e, field):
        save_rows(e, field)
        for copy in halo_copies(e):
            copy.start()

    def take_halo(e, field):
        for copy in halo_copies(e):
            copy.wait_recv()
        for which in (OUTER, INNER):
            field[which, SUB - 1:SUB] = rows_in[e, 0, which:which + 1]
            field[which, SUB + n_rows:SUB + n_rows + 1] = rows_in[e, 1, which:which + 1]

    def neighbours(e, field, which, j, sides=True):
        here = field[which, inside(j)]
        below = field[which, tile(j)]
        above = field[which, tile(j + 2)]
        to_south = jnp.where(wide == 0, pltpu.roll(below, 1, 0), pltpu.roll(here, 1, 0))
        to_north = jnp.where(
            wide == SUB - 1, pltpu.roll(above, SUB - 1, 0), pltpu.roll(here, SUB - 1, 0)
        )
        rows = pl.ds(which * SUB, SUB)
        from_west = from_east = 0.0
        if sides:
            from_west = pltpu.roll(cols_in[e, 0, rows], lax.rem(LANES - j, LANES), 1)
            from_east = pltpu.roll(cols_in[e, 1, rows], LANES - 1 - j, 1)
        shifted = pltpu.roll(here, 1, 1)
        to_west = jnp.concatenate(
            [jnp.where(lane == 0, from_west, shifted[:, :LANES]), shifted[:, LANES:]], axis=1
        )
        shifted = pltpu.roll(here, n_cols - 1, 1)
        to_east = jnp.concatenate(
            [shifted[:, :last], jnp.where(lane == LANES - 1, from_east, shifted[:, last:])], axis=1
        )
        return here, to_east, to_west, to_north, to_south

    for which in (OUTER, INNER):
        z2[which, :SUB] = jnp.zeros((SUB, n_cols), jnp.float32)
        z2[which, SUB + n_rows:] = jnp.zeros((SUB, n_cols), jnp.float32)

    loads[0].wait()
    table = halves(via_tab, INNER)

    def look_via(j):
        rv[tile(j)] = pick(via[layer[INNER], tile(j)], table)

    each(0, groups, look_via, 3)
    loads[1].wait()
    for which in (OUTER, INNER):
        plane_table = halves(plane_tab, which)

        def look_plane(j, which=which, plane_table=plane_table):
            found = pick(plane[layer[which], tile(j)], plane_table)
            rp[which, inside(j)] = found
            save_cols(0, which, j, found)

        each(0, groups, look_plane, 3)
    save_rows(0, rp)
    loads[2].wait()
    outer_table = halves(via_tab, OUTER)

    def look_outer(j):
        u_in[tile(j)] = 1.0 / (rv[tile(j)] + pick(via[layer[OUTER], tile(j)], outer_table))

    each(0, groups, look_outer, 3)
    for copy in loads[3:]:
        copy.wait()

    pl.semaphore_wait(barrier, len(nearby))
    for c in range(chunks):
        via_copy(c).start()
    for copy in halo_copies(0):
        copy.start()
    spread()
    top_pad = jnp.where(is_top, jnp.float32(PAD_CONDUCTANCE), jnp.float32(0.0))
    bottom_on = jnp.where(is_bottom, jnp.float32(1.0), jnp.float32(0.0))
    take_halo(0, rp)
    spread()
    near = lax.broadcasted_iota(jnp.int32, (2 * SUB, LANES), 1) < groups
    for i in range(2):
        both = jnp.where(near, cols_out[0, 1 - i] + cols_in[0, i], 1.0)
        side[i] = jnp.where(near, 1.0 / both, 0.0)

    def make_edges(j):
        for which in (OUTER, INNER):
            here, e, w, nn, s = neighbours(0, rp, which, j)
            total = None
            for i, other in enumerate((e, w, nn, s)):
                value = 1.0 / (here + other)
                edge[which, i, tile(j)] = value
                total = value if total is None else total + value
            total = total + u_in[tile(j)]
            if which == OUTER:
                total = total + top_pad * pad[tile(j)].astype(jnp.float32)
            dsum[which, tile(j)] = total
        b[tile(j)] = bottom_on * (sink[tile(j)].astype(jnp.float32) * load[tile(j)])

    each(0, groups, make_edges)

    @pl.when(is_bottom)
    def _():
        zx[0] = jnp.zeros_like(zx[0])

    def start_field(j):
        across = 1.0 / (rv[tile(j)] + rvx[tile(j)])
        ux[tile(j)] = across
        d_outer = dsum[OUTER, tile(j)]
        d_inner = dsum[INNER, tile(j)] + across
        joint = u_in[tile(j)]
        inverse = 1.0 / (d_outer * d_inner - joint * joint)
        oo, oi, ii = d_inner * inverse, joint * inverse, d_outer * inverse
        m[0, tile(j)] = oo
        m[1, tile(j)] = oi
        m[2, tile(j)] = ii
        source = b[tile(j)]
        for which, factor in ((OUTER, oo), (INNER, oi)):
            value = factor * source
            z0[which, inside(j)] = value
            save_cols(1, which, j, value)

    for c in range(chunks):
        via_copy(c).wait_recv()
        each(c * per, per, start_field)

        @pl.when(is_bottom)
        def _(c=c):
            field_copy(0, c).start()

    send_halo(1, z0)
    spread()

    def apply(k, j):
        out = []
        for which in (OUTER, INNER):
            here, e, w, nn, s = neighbours(k + 1, z[k], which, j, sides=k < 2)
            value = (
                edge[which, 0, tile(j)] * e + edge[which, 1, tile(j)] * w
                + edge[which, 2, tile(j)] * nn + edge[which, 3, tile(j)] * s
            )
            if which == INNER and k < 2:
                value = value + ux[tile(j)] * zx[k, tile(j)]
            n[k][which, tile(j)] = value
            out.append((here, value))
        return out

    def advance(k, j):
        (z_outer, n_outer), (z_inner, n_inner) = apply(k, j)
        oo, oi, ii = m[0, tile(j)], m[1, tile(j)], m[2, tile(j)]
        next_outer = oo * n_outer + oi * n_inner
        next_inner = oi * n_outer + ii * n_inner
        for which, value in ((OUTER, next_outer), (INNER, next_inner)):
            z[k + 1][which, inside(j)] = value
            save_cols(k + 2, which, j, value)
        if k == 0:
            acc[0] += fold(z_outer * b[tile(j)])
            acc[1] += fold(z_outer * n_outer + z_inner * n_inner)
            acc[2] += fold(next_outer * n_outer + next_inner * n_inner)
        else:
            acc[3] += fold(z_outer * n_outer + z_inner * n_inner)
            acc[4] += fold(next_outer * n_outer + next_inner * n_inner)

    for k in range(2):
        take_halo(k + 1, z[k])
        spread()
        for c in range(chunks):
            if k == 0:
                @pl.when(is_top)
                def _(c=c):
                    field_copy(0, c).wait_recv()
            else:
                field_copy(k, c).wait_recv()
            each(c * per, per, functools.partial(advance, k))
            if k == 0 or c < early:
                field_copy(k + 1, c).start()
            else:
                @pl.when(is_top)
                def _(c=c):
                    field_copy(2, c).start()
        send_halo(k + 2, z[k + 1])

    def finish(j):
        (z_outer, n_outer), (z_inner, n_inner) = apply(2, j)
        acc[5] += fold(z_outer * n_outer + z_inner * n_inner)

    each(0, groups, finish)
    while told[0] <= len(stages):
        spread()

    @pl.when(is_bottom)
    def _():
        def between(j):
            acc[5] += fold(2.0 * z2[INNER, inside(j)] * ux[tile(j)] * zx[2, tile(j)])

        for c in range(chunks):
            field_copy(2, c).wait_recv()
            each(c * per, per, between, 3)

    for copy in halo_copies(3):
        copy.wait_recv()
    end = n_rows - 1
    for i in range(2):
        side[i] = side[i] * cols_in[3, i]
    across_cols = cols_out[3, 1] * side[0] + cols_out[3, 0] * side[1]
    acc[5] += across_cols[:SUB] + across_cols[SUB:]
    for which in (OUTER, INNER):
        from_south = edge[which, 3, 0:1] * rows_in[3, 0, which:which + 1]
        from_north = edge[which, 2, end:n_rows] * rows_in[3, 1, which:which + 1]
        n2[which, 0:1] += from_south
        n2[which, end:n_rows] += from_north
        acc[5, 0:1] += fold(
            z2[which, SUB:SUB + 1] * from_south + z2[which, SUB + end:SUB + n_rows] * from_north
        )

    mix = jnp.zeros((SUB, LANES), jnp.float32)
    for k in range(6):
        total = jnp.sum(jnp.sum(acc[k], axis=0, keepdims=True), axis=1, keepdims=True)
        mix = jnp.where(lane == k, jnp.broadcast_to(total, (SUB, LANES)), mix)
    part[...] = mix[:1]
    red1[mine] = mix[:1]
    first = []
    for d, peer in enumerate(everyone):
        copy = pltpu.make_async_remote_copy(
            src_ref=part, dst_ref=red1.at[mine], send_sem=s1.at[d], recv_sem=r1.at[d],
            device_id=peer, device_id_type=MESH,
        )
        copy.start()
        first.append(copy)

    @pl.when(is_bottom)
    def _():
        for c in range(early, chunks):
            field_copy(2, c).start()

    def mend(j):
        for which in (OUTER, INNER):
            rows = pl.ds(which * SUB, SUB)
            from_west = pltpu.roll(side[0, rows], lax.rem(LANES - j, LANES), 1)
            from_east = pltpu.roll(side[1, rows], LANES - 1 - j, 1)
            n2[which, tile(j), :LANES] += jnp.where(lane == 0, from_west, 0.0)
            n2[which, tile(j), last:] += jnp.where(lane == LANES - 1, from_east, 0.0)

    each(0, groups, mend)
    for copy in first:
        copy.wait_recv()
    mix = red1[0]
    for i in range(1, total_count):
        mix = mix + red1[i]
    nu = [jnp.broadcast_to(mix[0:1, k:k + 1], (SUB, LANES)) for k in range(6)]
    h = [nu[k] - nu[k + 1] for k in range(5)]
    l10 = h[1] / h[0]
    d1 = h[2] - l10 * h[1]
    l20 = h[2] / h[0]
    t = h[3] - l10 * h[2]
    l21 = t / d1
    d2 = h[4] - l20 * h[2] - l21 * t
    y0 = nu[0]
    y1 = nu[1] - l10 * y0
    y2 = nu[2] - l20 * y0 - l21 * y1
    c2 = y2 / d2
    c1 = y1 / d1 - l21 * c2
    c0 = y0 / h[0] - l10 * c1 - l20 * c2

    def full(x):
        return jnp.concatenate([x] * (n_cols // LANES), axis=1)

    w0, w1, w2 = full(c0), full(c1), full(c2)
    rb, r0, rr1 = 1.0 - w0, w0 - w1, w1 - w2

    def emit(j):
        for which in (OUTER, INNER):
            volt[layer[which], tile(j)] = (
                w0 * z0[which, inside(j)] + w1 * z1[which, inside(j)]
                + w2 * z2[which, inside(j)]
            )
            tail = n2[which, tile(j)]
            if which == INNER:
                tail = tail + ux[tile(j)] * zx[2, tile(j)]
            value = r0 * n0[which, tile(j)] + rr1 * n1[which, tile(j)] + w2 * tail
            if which == OUTER:
                value = value + rb * b[tile(j)]
            res[layer[which], tile(j)] = value

    for c in range(chunks):
        @pl.when(is_top)
        def _(c=c):
            field_copy(2, c).wait_recv()
        each(c * per, per, emit, 3)

    for c in range(chunks):
        via_copy(c).wait_send()

        @pl.when(is_bottom)
        def _(c=c):
            field_copy(0, c).wait_send()
        field_copy(1, c).wait_send()
        field_copy(2, c).wait_send()
    for e in range(4):
        for copy in halo_copies(e):
            copy.wait_send()
    for copy in first:
        copy.wait_send()


def store(volt, res, volt_hbm, res_hbm, sem):
    copies = [
        pltpu.make_async_copy(src.at[k], dst.at[k], sem.at[i, k])
        for i, (src, dst) in enumerate(((volt, volt_hbm), (res, res_hbm)))
        for k in range(src.shape[0])
    ]
    for copy in copies:
        copy.start()
    for copy in copies:
        copy.wait()


def solution(mesh):
    sizes = tuple(mesh.shape[a] for a in ("gx", "gy", "gz"))
    n_gx, n_gy, n_gz = sizes

    def shards(load_current, sink_mask, pad_mask, plane_class, via_class, plane_table, via_table):
        n_layers, rows, cols = plane_class.shape
        groups = rows // SUB
        assert n_layers == 2 and n_gz == 2 and groups <= LANES
        chunks = max(c for c in range(1, 9) if groups % c == 0)
        f32, i32 = jnp.float32, jnp.int32
        dma = pltpu.SemaphoreType.DMA
        hbm = pl.BlockSpec(memory_space=pl.ANY)
        vmem = pl.BlockSpec(memory_space=VMEM)
        shape = (n_layers, rows, cols)
        padded = (2, rows + 2 * SUB, cols)
        flat = VMEM((rows, cols), f32)
        volt, res = pl.pallas_call(
            functools.partial(kernel, sizes, chunks),
            out_shape=(VMEM(shape, f32), VMEM(shape, f32)),
            in_specs=[hbm] * 5 + [vmem] * 2,
            out_specs=(vmem, vmem),
            scratch_shapes=[
                flat, VMEM((rows, cols), i32), VMEM((rows, cols), i32),
                VMEM((2, rows, cols), i32), VMEM((2, rows, cols), i32),
                flat, flat, VMEM(padded, f32), VMEM((2, 4, rows, cols), f32),
                VMEM((2, rows, cols), f32), flat, flat, VMEM((3, rows, cols), f32), flat,
                VMEM(padded, f32), VMEM(padded, f32), VMEM(padded, f32),
                VMEM((3, rows, cols), f32), VMEM((2, rows, cols), f32),
                VMEM((2, rows, cols), f32), VMEM((2, rows, cols), f32),
                VMEM((4, 2, SUB, cols), f32), VMEM((4, 2, SUB, cols), f32),
                VMEM((4, 2, 2 * SUB, LANES), f32), VMEM((4, 2, 2 * SUB, LANES), f32),
                VMEM((2, 2 * SUB, LANES), f32),
                VMEM((6, SUB, LANES), f32), VMEM((1, LANES), f32),
                VMEM((n_gx * n_gy * n_gz, 1, LANES), f32),
                dma((6,)), dma((4, chunks)), dma((4, chunks)),
                dma((4, 4)), dma((4, 4)),
                dma((n_gx * n_gy * n_gz - 1,)), dma((n_gx * n_gy * n_gz - 1,)),
                pltpu.SemaphoreType.REGULAR((len(word_plan(sizes)) + 1,)),
            ],
            compiler_params=pltpu.CompilerParams(
                collective_id=0, has_side_effects=True, vmem_limit_bytes=60 * 1024 * 1024
            ),
            name="grid_cg",
        )(load_current, sink_mask, pad_mask, plane_class, via_class, plane_table, via_table)
        whole = jax.ShapeDtypeStruct(shape, f32)
        return pl.pallas_call(
            store,
            out_shape=(whole, whole),
            in_specs=[vmem] * 2,
            out_specs=(hbm, hbm),
            scratch_shapes=[dma((2, n_layers))],
            name="store",
        )(*(pltpu.with_memory_space_constraint(x, VMEM) for x in (volt, res)))

    in_specs = (
        P("gy", "gx"), P("gy", "gx"), P("gy", "gx"),
        P("gz", "gy", "gx"), P("gz", "gy", "gx"), P("gz", None), P("gz", None),
    )
    out_specs = (P("gz", "gy", "gx"), P("gz", "gy", "gx"))
    return jax.shard_map(shards, mesh=mesh, in_specs=in_specs, out_specs=out_specs, check_vma=False)
```

```python
import functools

import jax
import jax.numpy as jnp
from jax import lax
from jax.experimental import pallas as pl
from jax.experimental.pallas import tpu as pltpu
from jax.sharding import PartitionSpec as P

PAD_CONDUCTANCE = 20.0
MESH = pl.DeviceIdType.MESH
VMEM = pltpu.VMEM
LANES = 128
SUB = 8
OUTER, INNER = 0, 1


def word_plan(sizes):
    n_gx, n_gy, _ = sizes
    plan, reach = [], 1
    while reach < n_gx // 2:
        plan.append(("gx", reach))
        reach *= 2
    stride = 1
    while stride - 1 < n_gy // 2:
        plan.append(("gy", stride))
        stride *= 2
    return plan


def kernel(
    sizes, chunks,
    load_hbm, sink_hbm, pad_hbm, plane_hbm, via_hbm, plane_tab, via_tab,
    volt, res,
    load, sink, pad, plane, via,
    rv, rvx, rp, edge, dsum, ux, u_in, m, b, z0, z1, z2, zx, n0, n1, n2,
    rows_out, rows_in, cols_out, cols_in, side, passed, acc, part, red,
    load_sem, p_send, p_recv, h_send, h_recv, f_send, f_recv, s1, r1, ready,
):
    z, n = (z0, z1, z2), (n0, n1, n2)
    n_gx, n_gy, n_gz = sizes
    _, n_rows, n_cols = plane.shape
    groups = n_rows // SUB
    per = groups // chunks
    middle = chunks - 2
    early = chunks * 3 // 4 - 2
    span = per * SUB
    last = n_cols - LANES
    gx, gy, gz = lax.axis_index("gx"), lax.axis_index("gy"), lax.axis_index("gz")
    is_bottom = gz == 0
    is_top = gz == n_gz - 1
    layer = {OUTER: gz, INNER: 1 - gz}
    partner = {"gz": 1 - gz}
    east, west = {"gx": lax.rem(gx + 1, n_gx)}, {"gx": lax.rem(gx + n_gx - 1, n_gx)}
    north, south = {"gy": lax.rem(gy + 1, n_gy)}, {"gy": lax.rem(gy + n_gy - 1, n_gy)}

    loads = [
        pltpu.make_async_copy(src, dst, load_sem.at[i])
        for i, (src, dst) in enumerate(
            (
                (via_hbm.at[layer[INNER]], via.at[layer[INNER]]), (plane_hbm, plane),
                (via_hbm.at[layer[OUTER]], via.at[layer[OUTER]]),
                (pad_hbm, pad), (load_hbm, load), (sink_hbm, sink),
            )
        )
    ]
    for copy in loads:
        copy.start()

    total_count = n_gx * n_gy * n_gz
    mine = (gx * n_gy + gy) * n_gz + gz
    everyone = []
    for d in range(1, total_count):
        other = lax.rem(mine + d, total_count)
        everyone.append({
            "gx": other // (n_gy * n_gz), "gy": lax.rem(other // n_gz, n_gy),
            "gz": lax.rem(other, n_gz),
        })

    def around(axis, at, size, stride):
        ahead = {axis: lax.rem(at + stride, size)}
        behind = {axis: lax.rem(at + size - stride, size)}
        return [ahead] if 2 * stride == size else [ahead, behind]

    nearby = [partner] + around("gy", gy, n_gy, 1) + around("gx", gx, n_gx, 1)
    barrier = pltpu.get_barrier_semaphore()
    for peer in nearby:
        pl.semaphore_signal(barrier, inc=1, device_id=peer, device_id_type=MESH)

    stages = [around(axis, at, size, stride) for axis, at, size, stride in (
        ("gx", gx, n_gx, s) if a == "gx" else ("gy", gy, n_gy, s) for a, s in word_plan(sizes)
    )] + [[partner]]
    told = [0]

    def spread():
        if 0 < told[0] <= len(stages):
            pl.semaphore_wait(ready.at[told[0] - 1], len(stages[told[0] - 1]))
        if told[0] < len(stages):
            for peer in stages[told[0]]:
                pl.semaphore_signal(
                    ready.at[told[0]], inc=1, device_id=peer, device_id_type=MESH
                )
        told[0] += 1

    lane = lax.broadcasted_iota(jnp.int32, (SUB, LANES), 1)
    wide = lax.broadcasted_iota(jnp.int32, (SUB, n_cols), 0)
    acc[...] = jnp.zeros_like(acc)
    cols_out[...] = jnp.zeros_like(cols_out)
    rows_out[...] = jnp.zeros_like(rows_out)

    def tile(j):
        return pl.ds(pl.multiple_of(j * SUB, SUB), SUB)

    def inside(j):
        return pl.ds(pl.multiple_of(j * SUB + SUB, SUB), SUB)

    def each(first, count, body, unroll=1):
        def step(i, carry):
            for u in range(wide_step):
                body(first + i * wide_step + u)
            return carry

        wide_step = unroll if count % unroll == 0 else 1
        lax.fori_loop(0, count // wide_step, step, 0)

    def loop(count, body, first=0):
        def step(i, carry):
            body(i)
            return carry

        lax.fori_loop(first, count, step, 0)

    def end(i):
        return i * (chunks - 1)

    def halves(table, which):
        row = 0.5 / table[pl.ds(layer[which], 1), :]
        return [jnp.broadcast_to(row[:, k:k + 1], (SUB, LANES)) for k in range(table.shape[1])]

    def pick(classes, values):
        out = []
        for s in range(0, n_cols, LANES):
            c = classes[:, s:s + LANES]
            level = list(values)
            bit = 1
            while len(level) > 1:
                on = (c & bit) != 0
                level = [jnp.where(on, level[i + 1], level[i]) for i in range(0, len(level), 2)]
                bit *= 2
            out.append(level[0])
        return jnp.concatenate(out, axis=1)

    def fold(x):
        total = x[:, :LANES]
        for s in range(LANES, n_cols, LANES):
            total = total + x[:, s:s + LANES]
        return total

    def plane_copy(e, c, src, dst):
        return pltpu.make_async_remote_copy(
            src_ref=src, dst_ref=dst, send_sem=p_send.at[e, c], recv_sem=p_recv.at[e, c],
            device_id=partner, device_id_type=MESH,
        )

    def chunk(c, pad=0):
        return pl.ds(pl.multiple_of(pad + c * span, SUB), span)

    def via_copy(c):
        return plane_copy(0, c, rv.at[chunk(c)], rvx.at[chunk(c)])

    def field_copy(k, c):
        return plane_copy(
            k + 1, c, z[k].at[INNER, chunk(c, SUB)], zx.at[k, chunk(c)]
        )

    def save_cols(e, which, j, tiles):
        rows = pl.ds(which * SUB, SUB)
        here = lane == j
        right = pltpu.roll(tiles[:, last:], j + 1, 1)
        left = pltpu.roll(tiles[:, :LANES], j, 1)
        cols_out[e, 0, rows] = jnp.where(here, right, cols_out[e, 0, rows])
        cols_out[e, 1, rows] = jnp.where(here, left, cols_out[e, 1, rows])

    def halo_copies(e):
        made = []
        plan = (
            (rows_out.at[e, 0], rows_in.at[e, 0], north),
            (rows_out.at[e, 1], rows_in.at[e, 1], south),
            (cols_out.at[e, 0], cols_in.at[e, 0], east),
            (cols_out.at[e, 1], cols_in.at[e, 1], west),
        )
        for i, (src, dst, peer) in enumerate(plan):
            made.append(
                pltpu.make_async_remote_copy(
                    src_ref=src, dst_ref=dst, send_sem=h_send.at[e, i],
                    recv_sem=h_recv.at[e, i], device_id=peer, device_id_type=MESH,
                )
            )
        return made

    def save_rows(e, field):
        for which in (OUTER, INNER):
            rows_out[e, 0, which:which + 1] = field[which, SUB + n_rows - 1:SUB + n_rows]
            rows_out[e, 1, which:which + 1] = field[which, SUB:SUB + 1]

    def send_halo(e, field):
        save_rows(e, field)
        for copy in halo_copies(e):
            copy.start()

    def take_rows(e, field):
        for copy in halo_copies(e)[:2]:
            copy.wait_recv()
        for which in (OUTER, INNER):
            field[which, SUB - 1:SUB] = rows_in[e, 0, which:which + 1]
            field[which, SUB + n_rows:SUB + n_rows + 1] = rows_in[e, 1, which:which + 1]

    def take_cols(e):
        for copy in halo_copies(e)[2:]:
            copy.wait_recv()

    def take_halo(e, field):
        take_rows(e, field)
        take_cols(e)

    def pass_copies():
        return [
            pltpu.make_async_remote_copy(
                src_ref=cols_in.at[1, i, pl.ds(SUB, SUB)], dst_ref=passed.at[i],
                send_sem=f_send.at[i], recv_sem=f_recv.at[i],
                device_id=partner, device_id_type=MESH,
            )
            for i in range(2)
        ]

    def neighbours(e, field, which, j, sides=True):
        here = field[which, inside(j)]
        below = field[which, tile(j)]
        above = field[which, tile(j + 2)]
        to_south = jnp.where(wide == 0, pltpu.roll(below, 1, 0), pltpu.roll(here, 1, 0))
        to_north = jnp.where(
            wide == SUB - 1, pltpu.roll(above, SUB - 1, 0), pltpu.roll(here, SUB - 1, 0)
        )
        rows = pl.ds(which * SUB, SUB)
        from_west = from_east = 0.0
        if sides:
            from_west = pltpu.roll(cols_in[e, 0, rows], lax.rem(LANES - j, LANES), 1)
            from_east = pltpu.roll(cols_in[e, 1, rows], LANES - 1 - j, 1)
        shifted = pltpu.roll(here, 1, 1)
        to_west = jnp.concatenate(
            [jnp.where(lane == 0, from_west, shifted[:, :LANES]), shifted[:, LANES:]], axis=1
        )
        shifted = pltpu.roll(here, n_cols - 1, 1)
        to_east = jnp.concatenate(
            [shifted[:, :last], jnp.where(lane == LANES - 1, from_east, shifted[:, last:])], axis=1
        )
        return here, to_east, to_west, to_north, to_south

    for which in (OUTER, INNER):
        z2[which, :SUB] = jnp.zeros((SUB, n_cols), jnp.float32)
        z2[which, SUB + n_rows:] = jnp.zeros((SUB, n_cols), jnp.float32)

    loads[0].wait()
    table = halves(via_tab, INNER)

    def look_via(j):
        rv[tile(j)] = pick(via[layer[INNER], tile(j)], table)

    each(0, groups, look_via, 3)
    loads[1].wait()
    for which in (OUTER, INNER):
        plane_table = halves(plane_tab, which)

        def look_plane(j, which=which, plane_table=plane_table):
            found = pick(plane[layer[which], tile(j)], plane_table)
            rp[which, inside(j)] = found
            save_cols(0, which, j, found)

        each(0, groups, look_plane, 3)
    save_rows(0, rp)
    loads[2].wait()
    outer_table = halves(via_tab, OUTER)

    def look_outer(j):
        u_in[tile(j)] = 1.0 / (rv[tile(j)] + pick(via[layer[OUTER], tile(j)], outer_table))

    each(0, groups, look_outer, 3)
    for copy in loads[3:]:
        copy.wait()

    pl.semaphore_wait(barrier, len(nearby))
    for copy in halo_copies(0):
        copy.start()
    loop(chunks, lambda c: via_copy(c).start())
    spread()
    top_pad = jnp.where(is_top, jnp.float32(PAD_CONDUCTANCE), jnp.float32(0.0))
    top_on = jnp.where(is_top, jnp.float32(1.0), jnp.float32(0.0))
    bottom_on = jnp.where(is_bottom, jnp.float32(1.0), jnp.float32(0.0))
    take_halo(0, rp)
    spread()
    near = lax.broadcasted_iota(jnp.int32, (2 * SUB, LANES), 1) < groups
    for i in range(2):
        both = jnp.where(near, cols_out[0, 1 - i] + cols_in[0, i], 1.0)
        side[i] = jnp.where(near, 1.0 / both, 0.0)

    def make_edges(j):
        for which in (OUTER, INNER):
            here, e, w, nn, s = neighbours(0, rp, which, j)
            total = None
            for i, other in enumerate((e, w, nn, s)):
                value = 1.0 / (here + other)
                edge[which, i, tile(j)] = value
                total = value if total is None else total + value
            total = total + u_in[tile(j)]
            if which == OUTER:
                total = total + top_pad * pad[tile(j)].astype(jnp.float32)
            dsum[which, tile(j)] = total
        b[tile(j)] = bottom_on * (sink[tile(j)].astype(jnp.float32) * load[tile(j)])

    each(0, groups, make_edges, 3)
    spread()

    def start_field(j):
        across = 1.0 / (rv[tile(j)] + rvx[tile(j)])
        ux[tile(j)] = across
        d_outer = dsum[OUTER, tile(j)]
        d_inner = dsum[INNER, tile(j)] + across
        joint = u_in[tile(j)]
        inverse = 1.0 / (d_outer * d_inner - joint * joint)
        oo, oi, ii = d_inner * inverse, joint * inverse, d_outer * inverse
        m[0, tile(j)] = oo
        m[1, tile(j)] = oi
        m[2, tile(j)] = ii
        source = b[tile(j)]
        for which, factor in ((OUTER, oo), (INNER, oi)):
            value = factor * source
            z0[which, inside(j)] = value
            response = (m[1 + which, tile(j)] * across) * top_on
            save_cols(1, which, j, value + response)

    def open_chunk(c):
        via_copy(c).wait_recv()
        each(c * per, per, start_field, 3)

        @pl.when(is_bottom)
        def _():
            field_copy(0, c).start()

    loop(chunks, open_chunk)

    @pl.when(is_bottom)
    def _():
        send_halo(1, z0)

    @pl.when(is_top)
    def _():
        for copy in halo_copies(1)[2:]:
            copy.start()

    spread()

    def apply(k, j):
        out = []
        for which in (OUTER, INNER):
            here, e, w, nn, s = neighbours(k + 1, z[k], which, j, sides=k < 2)
            value = (
                edge[which, 0, tile(j)] * e + edge[which, 1, tile(j)] * w
                + edge[which, 2, tile(j)] * nn + edge[which, 3, tile(j)] * s
            )
            if which == INNER and k == 1:
                value = value + ux[tile(j)] * zx[k, tile(j)]
            n[k][which, tile(j)] = value
            out.append((here, value))
        return out

    def advance(k, j):
        (z_outer, n_outer), (z_inner, n_inner) = apply(k, j)
        oo, oi, ii = m[0, tile(j)], m[1, tile(j)], m[2, tile(j)]
        next_outer = oo * n_outer + oi * n_inner
        next_inner = oi * n_outer + ii * n_inner
        for which, value in ((OUTER, next_outer), (INNER, next_inner)):
            z[k + 1][which, inside(j)] = value
            save_cols(k + 2, which, j, value)
        if k == 0:
            acc[0] += fold(z_outer * b[tile(j)])
            acc[1] += fold(z_outer * n_outer + z_inner * n_inner)
            acc[2] += fold(next_outer * n_outer + next_inner * n_inner)
        else:
            acc[3] += fold(z_outer * n_outer + z_inner * n_inner)
            acc[4] += fold(next_outer * n_outer + next_inner * n_inner)

    def begin(j):
        joint = ux[tile(j)] * zx[0, tile(j)]
        n0[OUTER, tile(j)] = jnp.zeros_like(joint)
        n0[INNER, tile(j)] = joint
        inner = m[2, tile(j)] * joint
        z1[OUTER, inside(j)] = m[1, tile(j)] * joint
        z1[INNER, inside(j)] = inner
        acc[2] += fold(inner * joint)

    @pl.when(is_top)
    def _():
        def begin_chunk(c):
            field_copy(0, c).wait_recv()
            each(c * per, per, begin, 3)
            field_copy(1, c).start()

        loop(chunks, begin_chunk)
        save_rows(2, z1)
        for copy in halo_copies(2)[:2]:
            copy.start()
        take_cols(1)
        for i, copy in enumerate(pass_copies()):
            copy.wait_recv()
            cols_in[2, i] = cols_in[1, i] * jnp.concatenate([passed[i], passed[i]], axis=0)

    @pl.when(is_bottom)
    def _():
        take_halo(1, z0)
        for copy in pass_copies():
            copy.start()
        def first_chunk(c):
            each(c * per, per, functools.partial(advance, 0), 3)
            field_copy(1, c).start()

        loop(chunks, lambda i: first_chunk(lax.rem(i + 1, chunks)))
        send_halo(2, z1)
        take_cols(2)

    while told[0] <= len(stages):
        spread()

    def second_chunk(c):
        field_copy(1, c).wait_recv()
        each(c * per, per, functools.partial(advance, 1), 3)

        @pl.when(is_top)
        def _():
            field_copy(2, c).start()

    loop(middle, lambda i: second_chunk(i + 1))
    take_rows(2, z1)
    loop(2, lambda i: second_chunk(end(1 - i)))

    @pl.when(is_bottom)
    def _():
        loop(2, lambda i: field_copy(2, end(i)).start())
        loop(early, lambda i: field_copy(2, middle - i).start())

    send_halo(3, z2)

    def put(mix, k):
        total = jnp.sum(jnp.sum(acc[k], axis=0, keepdims=True), axis=1, keepdims=True)
        return jnp.where(lane == k, jnp.broadcast_to(total, (SUB, LANES)), mix)

    def sum_copies():
        return [
            pltpu.make_async_remote_copy(
                src_ref=part, dst_ref=red.at[mine], send_sem=s1.at[d], recv_sem=r1.at[d],
                device_id=peer, device_id_type=MESH,
            )
            for d, peer in enumerate(everyone)
        ]

    def finish(j):
        (z_outer, n_outer), (z_inner, n_inner) = apply(2, j)
        acc[5] += fold(z_outer * n_outer + z_inner * n_inner)

    each(0, groups, finish, 3)

    mix = jnp.zeros((SUB, LANES), jnp.float32)
    for k in range(5):
        mix = put(mix, k)

    def between(j):
        acc[5] += fold(2.0 * z2[INNER, inside(j)] * ux[tile(j)] * zx[2, tile(j)])

    def between_chunk(c):
        field_copy(2, c).wait_recv()
        each(c * per, per, between, 3)

    @pl.when(is_top)
    def _():
        loop(2, lambda i: between_chunk(end(i)))

    @pl.when(is_bottom)
    def _():
        loop(middle, lambda i: between_chunk(i + 1))

    for copy in halo_copies(3):
        copy.wait_recv()
    edge_row = n_rows - 1
    for i in range(2):
        side[i] = side[i] * cols_in[3, i]
    across_cols = cols_out[3, 1] * side[0] + cols_out[3, 0] * side[1]
    acc[5] += across_cols[:SUB] + across_cols[SUB:]
    for which in (OUTER, INNER):
        from_south = edge[which, 3, 0:1] * rows_in[3, 0, which:which + 1]
        from_north = edge[which, 2, edge_row:n_rows] * rows_in[3, 1, which:which + 1]
        n2[which, 0:1] += from_south
        n2[which, edge_row:n_rows] += from_north
        acc[5, 0:1] += fold(
            z2[which, SUB:SUB + 1] * from_south + z2[which, SUB + edge_row:SUB + n_rows] * from_north
        )

    mix = put(mix, 5)
    part[...] = mix[:1]
    red[mine] = mix[:1]
    sums = sum_copies()
    for copy in sums:
        copy.start()

    @pl.when(is_bottom)
    def _():
        loop(middle, lambda i: field_copy(2, middle - i).start(), early)

    def mend(j):
        for which in (OUTER, INNER):
            rows = pl.ds(which * SUB, SUB)
            from_west = pltpu.roll(side[0, rows], lax.rem(LANES - j, LANES), 1)
            from_east = pltpu.roll(side[1, rows], LANES - 1 - j, 1)
            n2[which, tile(j), :LANES] += jnp.where(lane == 0, from_west, 0.0)
            n2[which, tile(j), last:] += jnp.where(lane == LANES - 1, from_east, 0.0)

    each(0, groups, mend, 6)
    for copy in sums:
        copy.wait_recv()
    rows = [red[i] for i in range(total_count)]
    while len(rows) > 1:
        rows = [sum(rows[i:i + 2][1:], rows[i]) for i in range(0, len(rows), 2)]
    mix = rows[0]
    nu = [jnp.broadcast_to(mix[0:1, k:k + 1], (SUB, LANES)) for k in range(6)]
    h = [nu[k] - nu[k + 1] for k in range(5)]
    l10 = h[1] / h[0]
    d1 = h[2] - l10 * h[1]
    l20 = h[2] / h[0]
    t = h[3] - l10 * h[2]
    l21 = t / d1
    y0 = nu[0]
    y1 = nu[1] - l10 * y0
    y2 = nu[2] - l20 * y0 - l21 * y1
    c2 = y2 / (h[4] - l20 * h[2] - l21 * t)
    c1 = y1 / d1 - l21 * c2
    c0 = y0 / h[0] - l10 * c1 - l20 * c2

    def full(x):
        return jnp.concatenate([x] * (n_cols // LANES), axis=1)

    w0, w1, w2 = full(c0), full(c1), full(c2)
    rb, r0, rr1 = 1.0 - w0, w0 - w1, w1 - w2

    def emit(j):
        for which in (OUTER, INNER):
            volt[layer[which], tile(j)] = (
                w0 * z0[which, inside(j)] + w1 * z1[which, inside(j)]
                + w2 * z2[which, inside(j)]
            )
            tail = n2[which, tile(j)]
            if which == INNER:
                tail = tail + ux[tile(j)] * zx[2, tile(j)]
            value = r0 * n0[which, tile(j)] + rr1 * n1[which, tile(j)] + w2 * tail
            if which == OUTER:
                value = value + rb * b[tile(j)]
            res[layer[which], tile(j)] = value

    def emit_chunk(c, other):
        @pl.when(other)
        def _():
            field_copy(2, c).wait_recv()

        each(c * per, per, emit, 3)

    loop(2, lambda i: emit_chunk(end(i), is_bottom))
    loop(middle, lambda i: emit_chunk(middle - i, is_top))

    def drain(c):
        via_copy(c).wait_send()
        field_copy(1, c).wait_send()
        field_copy(2, c).wait_send()

        @pl.when(is_bottom)
        def _():
            field_copy(0, c).wait_send()

    loop(chunks, drain)
    for copy in halo_copies(0) + halo_copies(1)[2:] + halo_copies(2)[:2] + halo_copies(3):
        copy.wait_send()

    @pl.when(is_bottom)
    def _():
        for copy in halo_copies(1)[:2] + halo_copies(2)[2:] + pass_copies():
            copy.wait_send()

    for copy in sums:
        copy.wait_send()


def store(volt, res, volt_hbm, res_hbm, sem):
    copies = [
        pltpu.make_async_copy(src.at[k], dst.at[k], sem.at[i, k])
        for i, (src, dst) in enumerate(((volt, volt_hbm), (res, res_hbm)))
        for k in range(src.shape[0])
    ]
    for copy in copies:
        copy.start()
    for copy in copies:
        copy.wait()


def solution(mesh):
    sizes = tuple(mesh.shape[a] for a in ("gx", "gy", "gz"))
    n_gx, n_gy, n_gz = sizes

    def shards(load_current, sink_mask, pad_mask, plane_class, via_class, plane_table, via_table):
        n_layers, rows, cols = plane_class.shape
        groups = rows // SUB
        assert n_layers == 2 and n_gz == 2 and groups <= LANES
        chunks = max(c for c in range(3, 9) if groups % c == 0)
        f32, i32 = jnp.float32, jnp.int32
        dma = pltpu.SemaphoreType.DMA
        hbm = pl.BlockSpec(memory_space=pl.ANY)
        vmem = pl.BlockSpec(memory_space=VMEM)
        shape = (n_layers, rows, cols)
        padded = (2, rows + 2 * SUB, cols)
        flat = VMEM((rows, cols), f32)
        volt, res = pl.pallas_call(
            functools.partial(kernel, sizes, chunks),
            out_shape=(VMEM(shape, f32), VMEM(shape, f32)),
            in_specs=[hbm] * 5 + [vmem] * 2,
            out_specs=(vmem, vmem),
            scratch_shapes=[
                flat, VMEM((rows, cols), i32), VMEM((rows, cols), i32),
                VMEM((2, rows, cols), i32), VMEM((2, rows, cols), i32),
                flat, flat, VMEM(padded, f32), VMEM((2, 4, rows, cols), f32),
                VMEM((2, rows, cols), f32), flat, flat, VMEM((3, rows, cols), f32), flat,
                VMEM(padded, f32), VMEM(padded, f32), VMEM(padded, f32),
                VMEM((3, rows, cols), f32), VMEM((2, rows, cols), f32),
                VMEM((2, rows, cols), f32), VMEM((2, rows, cols), f32),
                VMEM((4, 2, SUB, cols), f32), VMEM((4, 2, SUB, cols), f32),
                VMEM((4, 2, 2 * SUB, LANES), f32), VMEM((4, 2, 2 * SUB, LANES), f32),
                VMEM((2, 2 * SUB, LANES), f32), VMEM((2, SUB, LANES), f32),
                VMEM((6, SUB, LANES), f32), VMEM((1, LANES), f32),
                VMEM((n_gx * n_gy * n_gz, 1, LANES), f32),
                dma((6,)), dma((4, chunks)), dma((4, chunks)),
                dma((4, 4)), dma((4, 4)), dma((2,)), dma((2,)),
                dma((n_gx * n_gy * n_gz - 1,)), dma((n_gx * n_gy * n_gz - 1,)),
                pltpu.SemaphoreType.REGULAR((len(word_plan(sizes)) + 1,)),
            ],
            compiler_params=pltpu.CompilerParams(
                collective_id=0, has_side_effects=True, vmem_limit_bytes=60 * 1024 * 1024
            ),
            name="grid_cg",
        )(load_current, sink_mask, pad_mask, plane_class, via_class, plane_table, via_table)
        whole = jax.ShapeDtypeStruct(shape, f32)
        return pl.pallas_call(
            store,
            out_shape=(whole, whole),
            in_specs=[vmem] * 2,
            out_specs=(hbm, hbm),
            scratch_shapes=[dma((2, n_layers))],
            name="store",
        )(*(pltpu.with_memory_space_constraint(x, VMEM) for x in (volt, res)))

    in_specs = (
        P("gy", "gx"), P("gy", "gx"), P("gy", "gx"),
        P("gz", "gy", "gx"), P("gz", "gy", "gx"), P("gz", None), P("gz", None),
    )
    out_specs = (P("gz", "gy", "gx"), P("gz", "gy", "gx"))
    return jax.shard_map(shards, mesh=mesh, in_specs=in_specs, out_specs=out_specs, check_vma=False)
```

```python
import functools

import jax
import jax.numpy as jnp
from jax import lax
from jax.experimental import pallas as pl
from jax.experimental.pallas import tpu as pltpu
from jax.sharding import PartitionSpec as P

PAD_CONDUCTANCE = 20.0
MESH = pl.DeviceIdType.MESH
VMEM = pltpu.VMEM
LANES = 128
SUB = 8
OUTER, INNER = 0, 1


def word_plan(sizes):
    n_gx, n_gy, _ = sizes
    plan, reach = [], 1
    while reach < n_gx // 2:
        plan.append(("gx", reach))
        reach *= 2
    stride = 1
    while stride - 1 < n_gy // 2:
        plan.append(("gy", stride))
        stride *= 2
    return plan


def kernel(
    sizes, chunks,
    load_hbm, sink_hbm, pad_hbm, plane_hbm, via_hbm, plane_tab, via_tab,
    volt, res,
    load, sink, pad, plane, via,
    rv, rvx, rp, edge, dsum, ux, u_in, m, b, z0, z1, z2, zx, n0, n1, n2,
    rows_out, rows_in, cols_out, cols_in, side, passed, acc, part, red,
    load_sem, p_send, p_recv, h_send, h_recv, f_send, f_recv, s1, r1, ready,
):
    z, n = (z0, z1, z2), (n0, n1, n2)
    n_gx, n_gy, n_gz = sizes
    _, n_rows, n_cols = plane.shape
    groups = n_rows // SUB
    per = groups // chunks
    middle = chunks - 2
    early = middle // 3
    span = per * SUB
    last = n_cols - LANES
    gx, gy, gz = lax.axis_index("gx"), lax.axis_index("gy"), lax.axis_index("gz")
    is_bottom = gz == 0
    is_top = gz == n_gz - 1
    layer = {OUTER: gz, INNER: 1 - gz}
    partner = {"gz": 1 - gz}
    east, west = {"gx": lax.rem(gx + 1, n_gx)}, {"gx": lax.rem(gx + n_gx - 1, n_gx)}
    north, south = {"gy": lax.rem(gy + 1, n_gy)}, {"gy": lax.rem(gy + n_gy - 1, n_gy)}

    loads = [
        pltpu.make_async_copy(src, dst, load_sem.at[i])
        for i, (src, dst) in enumerate(
            (
                (via_hbm.at[layer[INNER]], via.at[layer[INNER]]), (plane_hbm, plane),
                (via_hbm.at[layer[OUTER]], via.at[layer[OUTER]]),
                (pad_hbm, pad), (load_hbm, load), (sink_hbm, sink),
            )
        )
    ]
    for copy in loads:
        copy.start()

    total_count = n_gx * n_gy * n_gz
    mine = (gx * n_gy + gy) * n_gz + gz
    everyone = []
    for d in range(1, total_count):
        other = lax.rem(mine + d, total_count)
        everyone.append({
            "gx": other // (n_gy * n_gz), "gy": lax.rem(other // n_gz, n_gy),
            "gz": lax.rem(other, n_gz),
        })

    def around(axis, at, size, stride):
        ahead = {axis: lax.rem(at + stride, size)}
        behind = {axis: lax.rem(at + size - stride, size)}
        return [ahead] if 2 * stride == size else [ahead, behind]

    nearby = [partner] + around("gy", gy, n_gy, 1) + around("gx", gx, n_gx, 1)
    barrier = pltpu.get_barrier_semaphore()
    for peer in nearby:
        pl.semaphore_signal(barrier, inc=1, device_id=peer, device_id_type=MESH)

    stages = [around(axis, at, size, stride) for axis, at, size, stride in (
        ("gx", gx, n_gx, s) if a == "gx" else ("gy", gy, n_gy, s) for a, s in word_plan(sizes)
    )] + [[partner]]
    told = [0]

    def spread():
        if 0 < told[0] <= len(stages):
            pl.semaphore_wait(ready.at[told[0] - 1], len(stages[told[0] - 1]))
        if told[0] < len(stages):
            for peer in stages[told[0]]:
                pl.semaphore_signal(
                    ready.at[told[0]], inc=1, device_id=peer, device_id_type=MESH
                )
        told[0] += 1

    lane = lax.broadcasted_iota(jnp.int32, (SUB, LANES), 1)
    wide = lax.broadcasted_iota(jnp.int32, (SUB, n_cols), 0)
    acc[...] = jnp.zeros_like(acc)
    cols_out[...] = jnp.zeros_like(cols_out)
    rows_out[...] = jnp.zeros_like(rows_out)

    def tile(j):
        return pl.ds(pl.multiple_of(j * SUB, SUB), SUB)

    def inside(j):
        return pl.ds(pl.multiple_of(j * SUB + SUB, SUB), SUB)

    def each(first, count, body, unroll=1):
        def step(i, carry):
            for u in range(wide_step):
                body(first + i * wide_step + u)
            return carry

        wide_step = unroll if count % unroll == 0 else 1
        lax.fori_loop(0, count // wide_step, step, 0)

    def loop(count, body, first=0):
        def step(i, carry):
            body(i)
            return carry

        lax.fori_loop(first, count, step, 0)

    def end(i):
        return i * (chunks - 1)

    def halves(table, which):
        row = 0.5 / table[pl.ds(layer[which], 1), :]
        return [jnp.broadcast_to(row[:, k:k + 1], (SUB, LANES)) for k in range(table.shape[1])]

    def pick(classes, values):
        out = []
        for s in range(0, n_cols, LANES):
            c = classes[:, s:s + LANES]
            level = list(values)
            bit = 1
            while len(level) > 1:
                on = (c & bit) != 0
                level = [jnp.where(on, level[i + 1], level[i]) for i in range(0, len(level), 2)]
                bit *= 2
            out.append(level[0])
        return jnp.concatenate(out, axis=1)

    def fold(x):
        total = x[:, :LANES]
        for s in range(LANES, n_cols, LANES):
            total = total + x[:, s:s + LANES]
        return total

    def plane_copy(e, c, src, dst):
        return pltpu.make_async_remote_copy(
            src_ref=src, dst_ref=dst, send_sem=p_send.at[e, c], recv_sem=p_recv.at[e, c],
            device_id=partner, device_id_type=MESH,
        )

    def chunk(c, pad=0):
        return pl.ds(pl.multiple_of(pad + c * span, SUB), span)

    def via_copy(c):
        return plane_copy(0, c, rv.at[chunk(c)], rvx.at[chunk(c)])

    def field_copy(k, c):
        return plane_copy(
            k + 1, c, z[k].at[INNER, chunk(c, SUB)], zx.at[k, chunk(c)]
        )

    def save_cols(e, which, j, tiles):
        rows = pl.ds(which * SUB, SUB)
        here = lane == j
        right = pltpu.roll(tiles[:, last:], j + 1, 1)
        left = pltpu.roll(tiles[:, :LANES], j, 1)
        cols_out[e, 0, rows] = jnp.where(here, right, cols_out[e, 0, rows])
        cols_out[e, 1, rows] = jnp.where(here, left, cols_out[e, 1, rows])

    def halo_copies(e):
        made = []
        plan = (
            (rows_out.at[e, 0], rows_in.at[e, 0], north),
            (rows_out.at[e, 1], rows_in.at[e, 1], south),
            (cols_out.at[e, 0], cols_in.at[e, 0], east),
            (cols_out.at[e, 1], cols_in.at[e, 1], west),
        )
        for i, (src, dst, peer) in enumerate(plan):
            made.append(
                pltpu.make_async_remote_copy(
                    src_ref=src, dst_ref=dst, send_sem=h_send.at[e, i],
                    recv_sem=h_recv.at[e, i], device_id=peer, device_id_type=MESH,
                )
            )
        return made

    def save_rows(e, field):
        for which in (OUTER, INNER):
            rows_out[e, 0, which:which + 1] = field[which, SUB + n_rows - 1:SUB + n_rows]
            rows_out[e, 1, which:which + 1] = field[which, SUB:SUB + 1]

    def send_halo(e, field):
        save_rows(e, field)
        for copy in halo_copies(e):
            copy.start()

    def take_rows(e, field):
        for copy in halo_copies(e)[:2]:
            copy.wait_recv()
        for which in (OUTER, INNER):
            field[which, SUB - 1:SUB] = rows_in[e, 0, which:which + 1]
            field[which, SUB + n_rows:SUB + n_rows + 1] = rows_in[e, 1, which:which + 1]

    def take_cols(e):
        for copy in halo_copies(e)[2:]:
            copy.wait_recv()

    def take_halo(e, field):
        take_rows(e, field)
        take_cols(e)

    def pass_copies():
        return [
            pltpu.make_async_remote_copy(
                src_ref=cols_in.at[1, i, pl.ds(SUB, SUB)], dst_ref=passed.at[i],
                send_sem=f_send.at[i], recv_sem=f_recv.at[i],
                device_id=partner, device_id_type=MESH,
            )
            for i in range(2)
        ]

    def neighbours(e, field, which, j, sides=True):
        here = field[which, inside(j)]
        below = field[which, tile(j)]
        above = field[which, tile(j + 2)]
        to_south = jnp.where(wide == 0, pltpu.roll(below, 1, 0), pltpu.roll(here, 1, 0))
        to_north = jnp.where(
            wide == SUB - 1, pltpu.roll(above, SUB - 1, 0), pltpu.roll(here, SUB - 1, 0)
        )
        rows = pl.ds(which * SUB, SUB)
        from_west = from_east = 0.0
        if sides:
            from_west = pltpu.roll(cols_in[e, 0, rows], lax.rem(LANES - j, LANES), 1)
            from_east = pltpu.roll(cols_in[e, 1, rows], LANES - 1 - j, 1)
        shifted = pltpu.roll(here, 1, 1)
        to_west = jnp.concatenate(
            [jnp.where(lane == 0, from_west, shifted[:, :LANES]), shifted[:, LANES:]], axis=1
        )
        shifted = pltpu.roll(here, n_cols - 1, 1)
        to_east = jnp.concatenate(
            [shifted[:, :last], jnp.where(lane == LANES - 1, from_east, shifted[:, last:])], axis=1
        )
        return here, to_east, to_west, to_north, to_south

    for which in (OUTER, INNER):
        z2[which, :SUB] = jnp.zeros((SUB, n_cols), jnp.float32)
        z2[which, SUB + n_rows:] = jnp.zeros((SUB, n_cols), jnp.float32)

    loads[0].wait()
    table = halves(via_tab, INNER)

    def look_via(j):
        rv[tile(j)] = pick(via[layer[INNER], tile(j)], table)

    each(0, groups, look_via, 3)
    pl.semaphore_wait(barrier, len(nearby))
    loop(chunks, lambda c: via_copy(c).start())
    spread()
    loads[1].wait()
    for which in (OUTER, INNER):
        plane_table = halves(plane_tab, which)

        def look_plane(j, which=which, plane_table=plane_table):
            found = pick(plane[layer[which], tile(j)], plane_table)
            rp[which, inside(j)] = found
            save_cols(0, which, j, found)

        each(0, groups, look_plane, 3)
    save_rows(0, rp)
    for copy in halo_copies(0):
        copy.start()
    loads[2].wait()
    outer_table = halves(via_tab, OUTER)

    def look_outer(j):
        u_in[tile(j)] = 1.0 / (rv[tile(j)] + pick(via[layer[OUTER], tile(j)], outer_table))

    each(0, groups, look_outer, 3)
    for copy in loads[3:]:
        copy.wait()

    top_pad = jnp.where(is_top, jnp.float32(PAD_CONDUCTANCE), jnp.float32(0.0))
    top_on = jnp.where(is_top, jnp.float32(1.0), jnp.float32(0.0))
    bottom_on = jnp.where(is_bottom, jnp.float32(1.0), jnp.float32(0.0))
    take_halo(0, rp)
    spread()
    near = lax.broadcasted_iota(jnp.int32, (2 * SUB, LANES), 1) < groups
    for i in range(2):
        both = jnp.where(near, cols_out[0, 1 - i] + cols_in[0, i], 1.0)
        side[i] = jnp.where(near, 1.0 / both, 0.0)

    def make_edges(j):
        for which in (OUTER, INNER):
            here, e, w, nn, s = neighbours(0, rp, which, j)
            total = None
            for i, other in enumerate((e, w, nn, s)):
                value = 1.0 / (here + other)
                edge[which, i, tile(j)] = value
                total = value if total is None else total + value
            total = total + u_in[tile(j)]
            if which == OUTER:
                total = total + top_pad * pad[tile(j)].astype(jnp.float32)
            dsum[which, tile(j)] = total
        b[tile(j)] = bottom_on * (sink[tile(j)].astype(jnp.float32) * load[tile(j)])

    each(0, groups, make_edges, 3)
    spread()

    def start_field(j):
        across = 1.0 / (rv[tile(j)] + rvx[tile(j)])
        ux[tile(j)] = across
        d_outer = dsum[OUTER, tile(j)]
        d_inner = dsum[INNER, tile(j)] + across
        joint = u_in[tile(j)]
        inverse = 1.0 / (d_outer * d_inner - joint * joint)
        oo, oi, ii = d_inner * inverse, joint * inverse, d_outer * inverse
        m[0, tile(j)] = oo
        m[1, tile(j)] = oi
        m[2, tile(j)] = ii
        source = b[tile(j)]
        for which, factor in ((OUTER, oo), (INNER, oi)):
            value = factor * source
            z0[which, inside(j)] = value
            response = (m[1 + which, tile(j)] * across) * top_on
            save_cols(1, which, j, value + response)

    def open_chunk(c):
        via_copy(c).wait_recv()
        each(c * per, per, start_field, 3)

        @pl.when(is_bottom)
        def _():
            field_copy(0, c).start()

    loop(chunks, open_chunk)

    @pl.when(is_bottom)
    def _():
        send_halo(1, z0)

    @pl.when(is_top)
    def _():
        for copy in halo_copies(1)[2:]:
            copy.start()

    spread()

    def apply(k, j):
        out = []
        for which in (OUTER, INNER):
            here, e, w, nn, s = neighbours(k + 1, z[k], which, j, sides=k < 2)
            value = (
                edge[which, 0, tile(j)] * e + edge[which, 1, tile(j)] * w
                + edge[which, 2, tile(j)] * nn + edge[which, 3, tile(j)] * s
            )
            if which == INNER and k == 1:
                value = value + ux[tile(j)] * zx[k, tile(j)]
            n[k][which, tile(j)] = value
            out.append((here, value))
        return out

    def advance(k, j):
        (z_outer, n_outer), (z_inner, n_inner) = apply(k, j)
        oo, oi, ii = m[0, tile(j)], m[1, tile(j)], m[2, tile(j)]
        next_outer = oo * n_outer + oi * n_inner
        next_inner = oi * n_outer + ii * n_inner
        for which, value in ((OUTER, next_outer), (INNER, next_inner)):
            z[k + 1][which, inside(j)] = value
            save_cols(k + 2, which, j, value)
        if k == 0:
            acc[0] += fold(z_outer * b[tile(j)])
            acc[1] += fold(z_outer * n_outer + z_inner * n_inner)
            acc[2] += fold(next_outer * n_outer + next_inner * n_inner)
        else:
            acc[3] += fold(z_outer * n_outer + z_inner * n_inner)
            acc[4] += fold(next_outer * n_outer + next_inner * n_inner)

    def begin(j):
        joint = ux[tile(j)] * zx[0, tile(j)]
        n0[OUTER, tile(j)] = jnp.zeros_like(joint)
        n0[INNER, tile(j)] = joint
        inner = m[2, tile(j)] * joint
        z1[OUTER, inside(j)] = m[1, tile(j)] * joint
        z1[INNER, inside(j)] = inner
        acc[2] += fold(inner * joint)

    @pl.when(is_top)
    def _():
        def begin_chunk(c):
            field_copy(0, c).wait_recv()
            each(c * per, per, begin, 3)
            field_copy(1, c).start()

        loop(chunks, begin_chunk)
        save_rows(2, z1)
        for copy in halo_copies(2)[:2]:
            copy.start()
        take_cols(1)
        for i, copy in enumerate(pass_copies()):
            copy.wait_recv()
            cols_in[2, i] = cols_in[1, i] * jnp.concatenate([passed[i], passed[i]], axis=0)

    @pl.when(is_bottom)
    def _():
        take_halo(1, z0)
        for copy in pass_copies():
            copy.start()
        def first_chunk(c):
            each(c * per, per, functools.partial(advance, 0), 3)
            field_copy(1, c).start()

        loop(chunks, lambda i: first_chunk(lax.rem(i + 1, chunks)))
        send_halo(2, z1)
        take_cols(2)

    while told[0] <= len(stages):
        spread()

    def second_chunk(c):
        field_copy(1, c).wait_recv()
        each(c * per, per, functools.partial(advance, 1), 3)

        @pl.when(is_top)
        def _():
            field_copy(2, c).start()

    loop(middle, lambda i: second_chunk(i + 1))
    take_rows(2, z1)
    loop(2, lambda i: second_chunk(end(1 - i)))

    @pl.when(is_bottom)
    def _():
        loop(2, lambda i: field_copy(2, end(i)).start())
        loop(early, lambda i: field_copy(2, middle - i).start())

    send_halo(3, z2)

    def put(mix, k):
        total = jnp.sum(jnp.sum(acc[k], axis=0, keepdims=True), axis=1, keepdims=True)
        return jnp.where(lane == k, jnp.broadcast_to(total, (SUB, LANES)), mix)

    def sum_copies():
        return [
            pltpu.make_async_remote_copy(
                src_ref=part, dst_ref=red.at[mine], send_sem=s1.at[d], recv_sem=r1.at[d],
                device_id=peer, device_id_type=MESH,
            )
            for d, peer in enumerate(everyone)
        ]

    def finish(j):
        (z_outer, n_outer), (z_inner, n_inner) = apply(2, j)
        acc[5] += fold(z_outer * n_outer + z_inner * n_inner)

    each(0, groups, finish, 3)

    mix = jnp.zeros((SUB, LANES), jnp.float32)
    for k in range(5):
        mix = put(mix, k)

    def between(j):
        acc[5] += fold(2.0 * z2[INNER, inside(j)] * ux[tile(j)] * zx[2, tile(j)])

    def between_chunk(c):
        field_copy(2, c).wait_recv()
        each(c * per, per, between, 3)

    @pl.when(is_top)
    def _():
        loop(2, lambda i: between_chunk(end(i)))

    @pl.when(is_bottom)
    def _():
        loop(middle, lambda i: between_chunk(i + 1))

    for copy in halo_copies(3):
        copy.wait_recv()
    edge_row = n_rows - 1
    for i in range(2):
        side[i] = side[i] * cols_in[3, i]
    across_cols = cols_out[3, 1] * side[0] + cols_out[3, 0] * side[1]
    acc[5] += across_cols[:SUB] + across_cols[SUB:]
    for which in (OUTER, INNER):
        from_south = edge[which, 3, 0:1] * rows_in[3, 0, which:which + 1]
        from_north = edge[which, 2, edge_row:n_rows] * rows_in[3, 1, which:which + 1]
        n2[which, 0:1] += from_south
        n2[which, edge_row:n_rows] += from_north
        acc[5, 0:1] += fold(
            z2[which, SUB:SUB + 1] * from_south + z2[which, SUB + edge_row:SUB + n_rows] * from_north
        )

    mix = put(mix, 5)
    part[...] = mix[:1]
    red[mine] = mix[:1]
    sums = sum_copies()
    for copy in sums:
        copy.start()

    @pl.when(is_bottom)
    def _():
        loop(middle, lambda i: field_copy(2, middle - i).start(), early)

    def mend(j):
        for which in (OUTER, INNER):
            rows = pl.ds(which * SUB, SUB)
            from_west = pltpu.roll(side[0, rows], lax.rem(LANES - j, LANES), 1)
            from_east = pltpu.roll(side[1, rows], LANES - 1 - j, 1)
            n2[which, tile(j), :LANES] += jnp.where(lane == 0, from_west, 0.0)
            n2[which, tile(j), last:] += jnp.where(lane == LANES - 1, from_east, 0.0)

    each(0, groups, mend, 6)
    for copy in sums:
        copy.wait_recv()
    rows = [red[i] for i in range(total_count)]
    while len(rows) > 1:
        rows = [sum(rows[i:i + 2][1:], rows[i]) for i in range(0, len(rows), 2)]
    mix = rows[0]
    nu = [jnp.broadcast_to(mix[0:1, k:k + 1], (SUB, LANES)) for k in range(6)]
    h = [nu[k] - nu[k + 1] for k in range(5)]
    l10 = h[1] / h[0]
    d1 = h[2] - l10 * h[1]
    l20 = h[2] / h[0]
    t = h[3] - l10 * h[2]
    l21 = t / d1
    y0 = nu[0]
    y1 = nu[1] - l10 * y0
    y2 = nu[2] - l20 * y0 - l21 * y1
    c2 = y2 / (h[4] - l20 * h[2] - l21 * t)
    c1 = y1 / d1 - l21 * c2
    c0 = y0 / h[0] - l10 * c1 - l20 * c2

    def full(x):
        return jnp.concatenate([x] * (n_cols // LANES), axis=1)

    w0, w1, w2 = full(c0), full(c1), full(c2)
    rb, r0, rr1 = 1.0 - w0, w0 - w1, w1 - w2

    def emit(j):
        for which in (OUTER, INNER):
            volt[layer[which], tile(j)] = (
                w0 * z0[which, inside(j)] + w1 * z1[which, inside(j)]
                + w2 * z2[which, inside(j)]
            )
            tail = n2[which, tile(j)]
            if which == INNER:
                tail = tail + ux[tile(j)] * zx[2, tile(j)]
            value = r0 * n0[which, tile(j)] + rr1 * n1[which, tile(j)] + w2 * tail
            if which == OUTER:
                value = value + rb * b[tile(j)]
            res[layer[which], tile(j)] = value

    def emit_chunk(c, other):
        @pl.when(other)
        def _():
            field_copy(2, c).wait_recv()

        each(c * per, per, emit, 3)

    loop(2, lambda i: emit_chunk(end(i), is_bottom))
    loop(middle, lambda i: emit_chunk(middle - i, is_top))

    def drain(c):
        via_copy(c).wait_send()
        field_copy(1, c).wait_send()
        field_copy(2, c).wait_send()

        @pl.when(is_bottom)
        def _():
            field_copy(0, c).wait_send()

    loop(chunks, drain)
    for copy in halo_copies(0) + halo_copies(1)[2:] + halo_copies(2)[:2] + halo_copies(3):
        copy.wait_send()

    @pl.when(is_bottom)
    def _():
        for copy in halo_copies(1)[:2] + halo_copies(2)[2:] + pass_copies():
            copy.wait_send()

    for copy in sums:
        copy.wait_send()


def store(volt, res, volt_hbm, res_hbm, sem):
    copies = [
        pltpu.make_async_copy(src.at[k], dst.at[k], sem.at[i, k])
        for i, (src, dst) in enumerate(((volt, volt_hbm), (res, res_hbm)))
        for k in range(src.shape[0])
    ]
    for copy in copies:
        copy.start()
    for copy in copies:
        copy.wait()


def solution(mesh):
    sizes = tuple(mesh.shape[a] for a in ("gx", "gy", "gz"))
    n_gx, n_gy, n_gz = sizes

    def shards(load_current, sink_mask, pad_mask, plane_class, via_class, plane_table, via_table):
        n_layers, rows, cols = plane_class.shape
        groups = rows // SUB
        assert n_layers == 2 and n_gz == 2 and groups <= LANES
        chunks = max(c for c in range(3, 9) if groups % c == 0)
        f32, i32 = jnp.float32, jnp.int32
        dma = pltpu.SemaphoreType.DMA
        hbm = pl.BlockSpec(memory_space=pl.ANY)
        vmem = pl.BlockSpec(memory_space=VMEM)
        shape = (n_layers, rows, cols)
        padded = (2, rows + 2 * SUB, cols)
        flat = VMEM((rows, cols), f32)
        volt, res = pl.pallas_call(
            functools.partial(kernel, sizes, chunks),
            out_shape=(VMEM(shape, f32), VMEM(shape, f32)),
            in_specs=[hbm] * 5 + [vmem] * 2,
            out_specs=(vmem, vmem),
            scratch_shapes=[
                flat, VMEM((rows, cols), i32), VMEM((rows, cols), i32),
                VMEM((2, rows, cols), i32), VMEM((2, rows, cols), i32),
                flat, flat, VMEM(padded, f32), VMEM((2, 4, rows, cols), f32),
                VMEM((2, rows, cols), f32), flat, flat, VMEM((3, rows, cols), f32), flat,
                VMEM(padded, f32), VMEM(padded, f32), VMEM(padded, f32),
                VMEM((3, rows, cols), f32), VMEM((2, rows, cols), f32),
                VMEM((2, rows, cols), f32), VMEM((2, rows, cols), f32),
                VMEM((4, 2, SUB, cols), f32), VMEM((4, 2, SUB, cols), f32),
                VMEM((4, 2, 2 * SUB, LANES), f32), VMEM((4, 2, 2 * SUB, LANES), f32),
                VMEM((2, 2 * SUB, LANES), f32), VMEM((2, SUB, LANES), f32),
                VMEM((6, SUB, LANES), f32), VMEM((1, LANES), f32),
                VMEM((n_gx * n_gy * n_gz, 1, LANES), f32),
                dma((6,)), dma((4, chunks)), dma((4, chunks)),
                dma((4, 4)), dma((4, 4)), dma((2,)), dma((2,)),
                dma((n_gx * n_gy * n_gz - 1,)), dma((n_gx * n_gy * n_gz - 1,)),
                pltpu.SemaphoreType.REGULAR((len(word_plan(sizes)) + 1,)),
            ],
            compiler_params=pltpu.CompilerParams(
                collective_id=0, has_side_effects=True, vmem_limit_bytes=60 * 1024 * 1024
            ),
            name="grid_cg",
        )(load_current, sink_mask, pad_mask, plane_class, via_class, plane_table, via_table)
        whole = jax.ShapeDtypeStruct(shape, f32)
        return pl.pallas_call(
            store,
            out_shape=(whole, whole),
            in_specs=[vmem] * 2,
            out_specs=(hbm, hbm),
            scratch_shapes=[dma((2, n_layers))],
            name="store",
        )(*(pltpu.with_memory_space_constraint(x, VMEM) for x in (volt, res)))

    in_specs = (
        P("gy", "gx"), P("gy", "gx"), P("gy", "gx"),
        P("gz", "gy", "gx"), P("gz", "gy", "gx"), P("gz", None), P("gz", None),
    )
    out_specs = (P("gz", "gy", "gx"), P("gz", "gy", "gx"))
    return jax.shard_map(shards, mesh=mesh, in_specs=in_specs, out_specs=out_specs, check_vma=False)
```
